32 devices in a mesh: blk: 4 (over y, x), half: 2 (over core), rep: 4 (over z).
Axes of the slice: x: 2, y: 2, z: 4, core: 2. Of those that a mesh axis runs over, the one named last changes fastest.
Arguments:
- tokens: bfloat16 [1024, 2048], P('blk'), may hold values from -6 to 6
- experts: int32 [1024, 6], P('blk'), may hold values from 0 to 63, all different within a row; in each aligned block of 256 rows (0 to 255, 256 to 511, ...) at most 32 rows name the same one
- gates: bfloat16 [1024, 6], P('blk'), may hold values from 0.099609375 to 1
- w_gate: bfloat16 [64, 1408, 2048], P('blk', ('half', 'rep')), may hold values from -0.125 to 0.125
- w_up: bfloat16 [64, 1408, 2048], P('blk', ('half', 'rep')), may hold values from -0.125 to 0.125
- w_down: bfloat16 [64, 1408, 2048], P('blk', ('half', 'rep')), may hold values from -0.15625 to 0.15625
- shared_gate: bfloat16 [1408, 2048], P(('half', 'rep')), may hold values from -0.125 to 0.125
- shared_up: bfloat16 [1408, 2048], P(('half', 'rep')), may hold values from -0.125 to 0.125
- shared_down: bfloat16 [1408, 2048], P(('half', 'rep')), may hold values from -0.15625 to 0.15625
Outputs:
- mixed: bfloat16 [1024, 2048], P('blk', ('half', 'rep'))
The draws below stay inside these ranges and needn't reach their ends.
Inputs may be any that keep to these rules, and one draw needn't show every extreme that they name: Each row names 6 different experts. Among the 256 rows held by one index of blk no expert is named by more than 32 rows, a bound that some block reaches.
All inputs are finite; a program needn't handle non-finite values.
Results may differ from the reference program's by a relative error of at most 0.0055.
Values may be sent and summed in bfloat16 or wider, within the bound.
No kernel may reach another device: no remote copies, remote signals or barrier semaphores. Data moves between devices by JAX's collectives and lax.ppermute only.
A program may use at most 128 MiB of HBM per device.

```python
import math
import jax
import jax.numpy as jnp
import numpy as np
from jax import lax

D = 2048
FF = 1408
E = 64
TOPK = 6
SH = 1408
TOK_DEV = 256
TOKENS = 1024
CAP = 32
N_BLK = 4
N_HALF = 2


def steps_of(stream_key, shape, shards, low, top_value):
    def one(dim, shards_of):
        draws = jax.random.uniform(jax.random.fold_in(jax.random.fold_in(stream_key, 6), dim), (shards_of,), jnp.float32, low / len(shards), top_value / len(shards))
        return jnp.repeat(jnp.exp(draws), shape[dim] // shards_of).reshape((-1,) + (1,) * (len(shape) - dim - 1))

    factor_of = one(*shards[0])
    for cut in shards[1:]:
        factor_of = factor_of * one(*cut)
    return factor_of


def routed_block(own_key, own, number, rows, amount, top, bound, slope):
    ranking = jax.random.permutation(own_key, amount)
    packed, common = shares(amount, rows * top, bound, slope, True), shares(amount, rows * top, bound, slope, False)
    places = jnp.arange(amount)

    def named(sizes, rotation):
        used = int((sizes > 0).sum())
        fixed = max(1, used // 4)
        moved = fixed + (places - fixed + rotation * (used - fixed)) % max(1, amount - fixed)
        return jnp.zeros((amount,), jnp.int32).at[ranking[jnp.where(places < fixed, places, moved)]].set(jnp.asarray(sizes, jnp.int32))

    sizes = jnp.where(number % 4 == 0, named(packed, number // 4), named(common, number - number // 4 - 1))
    mixed = jax.random.permutation(jax.random.fold_in(own, 3), amount)
    source_of, taker = mixed[0:amount // 2 * 2:2], mixed[1:amount // 2 * 2:2]
    margin = jnp.minimum(sizes[source_of] - 1, bound - sizes[taker]) // 2
    margin = jnp.where((source_of == ranking[0]) | (taker == ranking[0]) | (sizes[taker] == 0), 0, jnp.maximum(margin, 0))
    moved = jax.random.randint(jax.random.fold_in(own, 4), (amount // 2,), 0, 1 << 20) % (margin + 1)
    sizes = sizes.at[source_of].add(-moved).at[taker].add(moved)
    members = jnp.searchsorted(jnp.cumsum(sizes), jnp.arange(rows * top), side="right").astype(jnp.int32)
    listing = members.reshape(top, rows).T
    listing = listing[jax.random.permutation(jax.random.fold_in(own, 1), rows)]
    rotation = jax.random.randint(jax.random.fold_in(own, 2), (rows, 1), 0, top)
    return jnp.take_along_axis(listing, (jnp.arange(top)[None, :] + rotation) % top, axis=1)


def shares(amount, total, most, slope, full):
    weights = [(1 << 20) // math.isqrt(rank ** slope) + 1 for rank in range(1, amount + 1)]
    largest = most if full else min(most, max(-(-total // amount), total * weights[0] // sum(weights)))
    least = 1 if total - largest >= amount - 1 else 0
    counts, spare = [largest] + [least] * (amount - 1), total - largest - least * (amount - 1)
    while spare > 0:
        candidates = [i for i in range(1, amount) if counts[i] < largest] or [i for i in range(1, amount) if counts[i] < most]
        mass, remaining = sum([weights[i] for i in candidates]), spare
        for i in candidates:
            more = min(most - counts[i], max(1, remaining * weights[i] // mass), spare)
            counts[i] = counts[i] + more
            spare = spare - more
    return np.array(counts)


def noise(rng, shape, deviation, bound, shards=(), kind=jnp.bfloat16):
    values = deviation * jax.random.normal(rng, shape, jnp.float32)
    if shards:
        values = values * steps_of(rng, shape, shards, -0.22, 0.18)
    return jnp.clip(values, -bound, bound).astype(kind)


def setup_inputs(seed: int = 0) -> dict:
    key_list = jax.random.split(jax.random.key(seed), 10)
    tokens = noise(key_list[0], (TOKENS, D), 1.0, 6.0, ((0, 4),))
    experts_keys = jax.random.split(jax.random.fold_in(key_list[1], 1), TOKENS // TOK_DEV)
    experts_turns = jax.random.permutation(jax.random.fold_in(key_list[1], 3), TOKENS // TOK_DEV)
    experts = jax.vmap(lambda own, number: routed_block(jax.random.fold_in(key_list[1], 2), own, number, TOK_DEV, E, TOPK, CAP, 1))(experts_keys, experts_turns).reshape((TOKENS, TOPK))
    gates = jnp.clip(jnp.exp(math.log(1.0) - 2.306499 * jax.random.uniform(key_list[2], (TOKENS, TOPK), jnp.float32) ** steps_of(key_list[2], (TOKENS, TOPK), ((0, 4),), -0.2, 0.2)), 0.099609375, 1.0).astype(jnp.bfloat16)
    w_gate = noise(key_list[3], (E, FF, D), D ** -0.5, 0.125, ((0, 4), (1, 8)))
    w_up = noise(key_list[4], (E, FF, D), D ** -0.5, 0.125, ((0, 4), (1, 8)))
    w_down = noise(key_list[5], (E, FF, D), FF ** -0.5, 0.15625, ((0, 4), (1, 8)))
    shared_gate = noise(key_list[6], (SH, D), D ** -0.5, 0.125, ((0, 8),))
    shared_up = noise(key_list[7], (SH, D), D ** -0.5, 0.125, ((0, 8),))
    shared_down = noise(key_list[8], (SH, D), SH ** -0.5, 0.15625, ((0, 8),))
    return dict(tokens=tokens, experts=experts, gates=gates, w_gate=w_gate, w_up=w_up, w_down=w_down, shared_gate=shared_gate, shared_up=shared_up, shared_down=shared_down)


def reference(tokens, experts, gates, w_gate, w_up, w_down, shared_gate, shared_up, shared_down):
    blocks = N_HALF
    block_width = FF // blocks
    pairs = TOK_DEV * TOPK
    grouped = experts.reshape(N_BLK, pairs)
    onehot = (grouped[:, :, None] == jnp.arange(E, dtype=jnp.int32)[None, None, :]).astype(jnp.int32)
    before = jnp.cumsum(onehot, axis=1) - onehot
    ranks = jnp.sum(before * onehot, axis=2).astype(jnp.int32)
    source = jnp.arange(N_BLK, dtype=jnp.int32)[:, None]
    position = source * CAP + ranks
    token_ids = source * TOK_DEV + (jnp.arange(pairs, dtype=jnp.int32) // TOPK)[None, :]
    table = jnp.full((E, N_BLK * CAP), TOKENS, jnp.int32)
    table = table.at[grouped.reshape(-1), position.reshape(-1)].set(token_ids.reshape(-1).astype(jnp.int32))
    weight_table = jnp.zeros((E, N_BLK * CAP), jnp.float32)
    weight_table = weight_table.at[grouped.reshape(-1), position.reshape(-1)].set(gates.reshape(-1).astype(jnp.float32))

    def one_expert(carry, item):
        index, weights, gate_matrix, up_weight, down_w = item
        token_rows = jnp.take(tokens, index, axis=0, mode="fill", fill_value=0)
        gate_values = jnp.dot(token_rows, gate_matrix.T, preferred_element_type=jnp.float32)
        raised_rows = jnp.dot(token_rows, up_weight.T, preferred_element_type=jnp.float32)
        hidden_state = (jax.nn.silu(gate_values) * raised_rows).astype(jnp.bfloat16)
        count = hidden_state.shape[0]
        pieces = jnp.einsum("rkf,kfd->rkd", hidden_state.reshape(count, blocks, block_width).astype(jnp.float32),
                            down_w.reshape(blocks, block_width, D).astype(jnp.float32))
        rounded = lax.optimization_barrier(pieces.astype(jnp.bfloat16))
        summed = jnp.sum(rounded.astype(jnp.float32), axis=1)
        carry = carry.at[index].add(weights[:, None] * summed, mode="drop")
        return carry, None

    routed, _ = lax.scan(one_expert, jnp.zeros((TOKENS, D), jnp.float32),
                         (table, weight_table, w_gate, w_up, w_down))
    shared_hidden = (jax.nn.silu(jnp.dot(tokens, shared_gate.T, preferred_element_type=jnp.float32))
                     * jnp.dot(tokens, shared_up.T, preferred_element_type=jnp.float32)).astype(jnp.bfloat16)
    shared_output = jnp.dot(shared_hidden, shared_down, preferred_element_type=jnp.float32)
    return (routed + shared_output).astype(jnp.bfloat16)
```

```python
import functools

import jax
import jax.numpy as jnp
from jax import lax
from jax.experimental import pallas as pl
from jax.experimental.pallas import tpu as pltpu
from jax.sharding import PartitionSpec as P

E = 64
CAP = 32


def target(index, step, count):
    return index ^ step if count & (count - 1) == 0 else (index + step) % count


def origin(index, step, count):
    return index ^ step if count & (count - 1) == 0 else (index + count - step) % count


def send(value, axis, step, back=False):
    count = lax.axis_size(axis)
    where = origin if back else target
    return lax.ppermute(value, axis, [(i, where(i, step, count)) for i in range(count)])


def dot(left, right, dims):
    return lax.dot_general(left, right, (dims, ((), ())), preferred_element_type=jnp.float32)


ROWS = ((1,), (1,))
PLAIN = ((1,), (0,))
TURNED = ((0,), (0,))


def expert_kernel(blocks, group, half_ref, meta_ref, own_ref, *refs):
    arrived = refs[: 2 * (blocks - 1)]
    refs = refs[2 * (blocks - 1):]
    gate_ref, up_ref, down_ref, sgate_ref, sup_ref, sdown_ref = refs[:6]
    keeps = refs[6:6 + blocks]
    sends = refs[6 + blocks:6 + 2 * blocks]
    token_ref, row_ref, value_ref, total_ref = refs[6 + 2 * blocks:]
    outer, inner = pl.program_id(0), pl.program_id(1)
    half = half_ref[0]
    count = own_ref.shape[0]
    part = count // 2
    width = own_ref.shape[1]

    @pl.when((outer == 0) & (inner == 0))
    def _():
        tokens = own_ref[...]
        token_ref[0] = tokens
        for k in range(1, blocks):
            mine, other = arrived[2 * (k - 1)], arrived[2 * (k - 1) + 1]
            token_ref[k, pl.ds(pl.multiple_of(half * part, part), part), :] = mine[...]
            token_ref[k, pl.ds(pl.multiple_of((1 - half) * part, part), part), :] = other[...]
            total_ref[k] = jnp.zeros((count, width), jnp.float32)
        gate_values = dot(tokens, sgate_ref[...], ROWS)
        raised = dot(tokens, sup_ref[...], ROWS)
        hidden = (jax.nn.silu(gate_values) * raised).astype(jnp.bfloat16)
        total_ref[0] = dot(hidden, sdown_ref[...], PLAIN)

    def chosen(k):
        slots = meta_ref[k, 0]
        number = lax.broadcasted_iota(jnp.int32, (group, CAP, count), 1).astype(jnp.float32)
        return (slots[:, None, :] == number)

    @pl.when(inner == 0)
    def _():
        for k in range(blocks):
            pick = jnp.where(chosen(k), 1.0, 0.0).reshape(group * CAP, count).astype(jnp.bfloat16)
            rows = dot(pick, token_ref[k], PLAIN).astype(jnp.bfloat16)
            row_ref[:, k * CAP:(k + 1) * CAP, :] = rows.reshape(group, CAP, width)

    rows = row_ref[inner]
    gate_values = dot(rows, gate_ref[0], ROWS)
    raised = dot(rows, up_ref[0], ROWS)
    hidden = (jax.nn.silu(gate_values) * raised).astype(jnp.bfloat16)
    value = dot(hidden, down_ref[0], PLAIN).astype(jnp.bfloat16)
    for k in range(blocks):
        value_ref[k, inner] = value[k * CAP:(k + 1) * CAP]

    @pl.when(inner == group - 1)
    def _():
        for k in range(blocks):
            weight = jnp.where(chosen(k), meta_ref[k, 1][:, None, :], 0.0)
            weight = weight.reshape(group * CAP, count).astype(jnp.bfloat16)
            values = value_ref[k].reshape(group * CAP, width)
            total_ref[k] += dot(weight, values, TURNED)

    @pl.when((outer == pl.num_programs(0) - 1) & (inner == group - 1))
    def _():
        side = width // 2
        for k in range(blocks):
            keeps[k][...] = total_ref[k, :, pl.ds(pl.multiple_of(half * side, side), side)]
            sends[k][...] = total_ref[
                k, :, pl.ds(pl.multiple_of((1 - half) * side, side), side)
            ].astype(jnp.bfloat16)


def run_experts(half, meta, own, arrived, weights, shared):
    blocks = meta.shape[0]
    experts, units, width = weights[0].shape
    count = own.shape[0]
    group = next(g for g in (8, 4, 2, 1) if experts % g == 0)
    once = pl.Buffered(1)

    def whole(array):
        return pl.BlockSpec(
            array.shape, lambda o, i: (0,) * array.ndim, pipeline_mode=once
        )

    weight_spec = pl.BlockSpec((1, units, width), lambda o, i: (o * group + i, 0, 0))
    half_shape = (count, width // 2)
    out_spec = pl.BlockSpec(half_shape, lambda o, i: (0, 0), pipeline_mode=once)
    return pl.pallas_call(
        functools.partial(expert_kernel, blocks, group),
        grid=(experts // group, group),
        in_specs=[
            pl.BlockSpec(memory_space=pltpu.SMEM),
            pl.BlockSpec((blocks, 2, group, count), lambda o, i: (0, 0, o, 0)),
            whole(own),
            *[whole(a) for a in arrived],
            weight_spec,
            weight_spec,
            weight_spec,
            *[whole(s) for s in shared],
        ],
        out_specs=[out_spec] * (2 * blocks),
        out_shape=[jax.ShapeDtypeStruct(half_shape, jnp.float32)] * blocks
        + [jax.ShapeDtypeStruct(half_shape, jnp.bfloat16)] * blocks,
        scratch_shapes=[
            pltpu.VMEM((blocks, count, width), jnp.bfloat16),
            pltpu.VMEM((group, blocks * CAP, width), jnp.bfloat16),
            pltpu.VMEM((blocks, group, CAP, width), jnp.bfloat16),
            pltpu.VMEM((blocks, count, width), jnp.float32),
        ],
        compiler_params=pltpu.CompilerParams(
            dimension_semantics=("arbitrary", "arbitrary"), vmem_limit_bytes=60 * 2**20
        ),
    )(half, meta, own, *arrived, *weights, *shared)


def gathered_plan(tokens, experts, gates, w_gate, w_up, w_down, shared_gate, shared_up, shared_down):
    count, width = tokens.shape
    topk = experts.shape[1]
    exp_local = w_gate.shape[0]
    blocks = lax.axis_size("blk")
    reps = lax.axis_size("rep")
    blk, half, rep = lax.axis_index("blk"), lax.axis_index("half"), lax.axis_index("rep")

    piece = lax.dynamic_slice_in_dim(tokens, half * (count // 2), count // 2, 0)
    order = list(range(blocks - 1, 0, -1))
    mine = {k: send(piece, "blk", k) for k in order}

    turned = experts.T
    names = jnp.arange(E, dtype=jnp.int32)[:, None]
    named = jnp.zeros((E, count), jnp.float32)
    gate_of = jnp.zeros((E, count), jnp.float32)
    gates_turned = gates.astype(jnp.float32).T
    for j in range(topk):
        same = names == turned[j][None, :]
        named = jnp.where(same, 1.0, named)
        gate_of = jnp.where(same, gates_turned[j][None, :], gate_of)
    index = jnp.arange(count, dtype=jnp.int32)
    earlier = (index[:, None] < index[None, :]).astype(jnp.bfloat16)
    ranks = jnp.dot(named.astype(jnp.bfloat16), earlier, preferred_element_type=jnp.float32)
    slots = jnp.where(named > 0, ranks, -1.0)
    meta = jnp.stack([slots, gate_of]).astype(jnp.bfloat16)

    def for_block(b):
        return lax.dynamic_slice_in_dim(meta, b * exp_local, exp_local, 1)

    metas = [for_block(blk)]
    for k in range(1, blocks):
        metas.append(send(for_block(target(blk, k, blocks)), "blk", k))
    other = {k: send(mine[k], "half", 1) for k in order}
    arrived = [a for k in range(1, blocks) for a in (mine[k], other[k])]

    outs = run_experts(
        half.astype(jnp.int32).reshape(1),
        jnp.stack(metas).astype(jnp.float32),
        tokens,
        arrived,
        (w_gate, w_up, w_down),
        (shared_gate, shared_up, shared_down),
    )
    keeps, sends = outs[:blocks], outs[blocks:]
    back = {}
    for k in order:
        joined = keeps[k] + send(sends[k], "half", 1).astype(jnp.float32)
        back[k] = send(joined.astype(jnp.bfloat16), "blk", k, back=True)
    total = keeps[0] + send(sends[0], "half", 1).astype(jnp.float32)
    for k in order:
        total = total + back[k].astype(jnp.float32)
    side = total.shape[1] // reps

    def for_rep(r):
        return lax.dynamic_slice_in_dim(total, r * side, side, 1)

    result = for_rep(rep)
    for k in range(reps - 1, 0, -1):
        share = for_rep(target(rep, k, reps)).astype(jnp.bfloat16)
        result = result + send(share, "rep", k).astype(jnp.float32)
    return result.astype(jnp.bfloat16)


def hidden_units(token_rows, gate_matrix, up_weight):
    gate_values = jnp.einsum(
        "kan,ktn->kat", token_rows, gate_matrix, preferred_element_type=jnp.float32
    )
    raised_rows = jnp.einsum(
        "kan,ktn->kat", token_rows, up_weight, preferred_element_type=jnp.float32
    )
    return (jax.nn.silu(gate_values) * raised_rows).astype(jnp.bfloat16)


def place_slots(flat, ranks, block_size, which, slot_count):
    inside = ranks // block_size == which
    local = jnp.where(inside, flat * block_size + ranks % block_size, -1)
    return local[:, None] == jnp.arange(slot_count, dtype=jnp.int32)[None, :]


def slotted_plan(tokens, experts, gates, w_gate, w_up, w_down, shared_gate, shared_up, shared_down):
    token_count = tokens.shape[0]
    width = tokens.shape[1]
    topk = experts.shape[1]
    exp_local = w_gate.shape[0]
    blk_count = lax.axis_size("blk")
    slot_block = CAP // lax.axis_size("rep")
    member_rep = lax.axis_index("rep")
    flat = experts.reshape(-1)
    onehot = (flat[:, None] == jnp.arange(E, dtype=jnp.int32)[None, :]).astype(jnp.int32)
    before = jnp.cumsum(onehot, axis=0) - onehot
    ranks = jnp.sum(before * onehot, axis=1)
    placing = place_slots(flat, ranks, slot_block, member_rep, E * slot_block).reshape(
        token_count, topk, -1
    )
    weighting = jnp.sum(
        placing.astype(jnp.float32) * gates.astype(jnp.float32)[:, :, None], axis=1
    ).astype(jnp.bfloat16)
    selector = jnp.any(placing, axis=1).astype(jnp.bfloat16)
    filled = jnp.einsum("ts,td->sd", selector, tokens, preferred_element_type=jnp.float32).astype(
        jnp.bfloat16
    )
    filled = filled.reshape(E, 1, slot_block, width)
    arrived = lax.all_to_all(filled, "blk", split_axis=0, concat_axis=1, tiled=True)
    token_rows = arrived.reshape(exp_local, -1, width)
    every_hidden = hidden_units(lax.all_gather(token_rows, "rep", axis=1, tiled=True), w_gate, w_up)
    mine = lax.all_to_all(every_hidden, "rep", split_axis=1, concat_axis=2, tiled=True)
    partial_value = jnp.einsum(
        "otv,ovj->otj",
        mine,
        lax.all_gather(w_down, "rep", axis=1, tiled=True),
        preferred_element_type=jnp.float32,
    )
    block_out = partial_value.astype(jnp.bfloat16).reshape(exp_local, blk_count, slot_block, width)
    returned = lax.all_to_all(block_out, "blk", split_axis=1, concat_axis=0, tiled=True)
    returned = returned.reshape(E * slot_block, width)
    routed = jnp.dot(weighting, returned, preferred_element_type=jnp.float32)
    shared_hidden = (
        jax.nn.silu(
            jnp.einsum("td,sd->ts", tokens, shared_gate, preferred_element_type=jnp.float32)
        )
        * jnp.einsum("td,sd->ts", tokens, shared_up, preferred_element_type=jnp.float32)
    ).astype(jnp.bfloat16)
    shared_output = jnp.dot(shared_hidden, shared_down, preferred_element_type=jnp.float32)
    routed_share = lax.psum_scatter(routed, ("half", "rep"), scatter_dimension=1, tiled=True)
    shared_share = lax.psum_scatter(shared_output, ("half", "rep"), scatter_dimension=1, tiled=True)
    total = routed_share + shared_share
    return total.astype(jnp.bfloat16)


def per_device(*args):
    tokens, w_gate = args[0], args[3]
    blocks = lax.axis_size("blk")
    gathered_rows = blocks * tokens.shape[0]
    slot_rows = w_gate.shape[0] * blocks * CAP
    if gathered_rows <= slot_rows and lax.axis_size("half") == 2:
        return gathered_plan(*args)
    return slotted_plan(*args)


def solution(mesh):
    return jax.shard_map(
        per_device,
        mesh=mesh,
        in_specs=(
            P("blk", None),
            P("blk", None),
            P("blk", None),
            P("blk", ("half", "rep"), None),
            P("blk", ("half", "rep"), None),
            P("blk", ("half", "rep"), None),
            P(("half", "rep"), None),
            P(("half", "rep"), None),
            P(("half", "rep"), None),
        ),
        out_specs=P("blk", ("half", "rep")),
        check_vma=False,
    )
```

```python
import functools

import jax
import jax.numpy as jnp
from jax import lax
from jax.experimental import pallas as pl
from jax.experimental.pallas import tpu as pltpu
from jax.sharding import PartitionSpec as P

E = 64
CAP = 32


def target(index, step, count):
    return index ^ step if count & (count - 1) == 0 else (index + step) % count


def send(value, axis, step):
    count = lax.axis_size(axis)
    return lax.ppermute(value, axis, [(i, target(i, step, count)) for i in range(count)])


def dot(left, right, dims):
    return lax.dot_general(left, right, (dims, ((), ())), preferred_element_type=jnp.float32)


ROWS = ((1,), (1,))
PLAIN = ((1,), (0,))
TURNED = ((0,), (0,))


FIRST_X, FIRST_Y, LAST_X, LAST_Y = range(4)
PIECES = (((1, 3), 0), ((2, 3), 1), ((0, 2), 0), ((0, 1), 1))


def expert_kernel(blocks, group, places, half_ref, meta_ref, own_ref, *refs):
    arrived = refs[: len(places)]
    refs = refs[len(places):]
    gate_ref, up_ref, down_ref, sgate_ref, sup_ref, sdown_ref = refs[:6]
    keeps = refs[6:6 + len(PIECES)]
    sends = refs[6 + len(PIECES):6 + 2 * len(PIECES)]
    token_ref, row_ref, value_ref, total_ref = refs[6 + 2 * len(PIECES):]
    outer, inner = pl.program_id(0), pl.program_id(1)
    half = half_ref[0]
    count = own_ref.shape[0]
    part = count // 2
    width = own_ref.shape[1]

    @pl.when((outer == 0) & (inner == 0))
    def _():
        tokens = own_ref[...]
        token_ref[0] = tokens
        for ref, (k, other, first) in zip(arrived, places):
            side = 1 - half if other else half
            length = ref.shape[0]
            start = pl.multiple_of(side * part + first, length)
            token_ref[k, pl.ds(start, length), :] = ref[...]
        for k in range(1, blocks):
            total_ref[k] = jnp.zeros((count, width), jnp.float32)
        gate_values = dot(tokens, sgate_ref[...], ROWS)
        raised = dot(tokens, sup_ref[...], ROWS)
        hidden = (jax.nn.silu(gate_values) * raised).astype(jnp.bfloat16)
        total_ref[0] = dot(hidden, sdown_ref[...], PLAIN)

    def chosen(k):
        slots = meta_ref[k, 0]
        number = lax.broadcasted_iota(jnp.int32, (group, CAP, count), 1).astype(jnp.float32)
        return (slots[:, None, :] == number)

    @pl.when(inner == 0)
    def _():
        for k in range(blocks):
            pick = jnp.where(chosen(k), 1.0, 0.0).reshape(group * CAP, count).astype(jnp.bfloat16)
            rows = dot(pick, token_ref[k], PLAIN).astype(jnp.bfloat16)
            row_ref[:, k * CAP:(k + 1) * CAP, :] = rows.reshape(group, CAP, width)

    pair = gate_ref.shape[0]
    for u in range(pair):
        rows = row_ref[inner * pair + u]
        gate_values = dot(rows, gate_ref[u], ROWS)
        raised = dot(rows, up_ref[u], ROWS)
        hidden = (jax.nn.silu(gate_values) * raised).astype(jnp.bfloat16)
        value = dot(hidden, down_ref[u], PLAIN).astype(jnp.bfloat16)
        for k in range(blocks):
            value_ref[k, inner * pair + u] = value[k * CAP:(k + 1) * CAP]

    @pl.when(inner == pl.num_programs(1) - 1)
    def _():
        for k in range(blocks):
            weight = jnp.where(chosen(k), meta_ref[k, 1][:, None, :], 0.0)
            weight = weight.reshape(group * CAP, count).astype(jnp.bfloat16)
            values = value_ref[k].reshape(group * CAP, width)
            total_ref[k] += dot(weight, values, TURNED)

    @pl.when((outer == pl.num_programs(0) - 1) & (inner == pl.num_programs(1) - 1))
    def _():
        side = width // 4
        for p, (members, column) in enumerate(PIECES):
            here = pl.ds(pl.multiple_of((2 * half + column) * side, side), side)
            there = pl.ds(pl.multiple_of((2 - 2 * half + column) * side, side), side)
            for j, k in enumerate(members):
                keeps[p][j] = total_ref[k, :, here]
                sends[p][j] = total_ref[k, :, there].astype(jnp.bfloat16)


def run_experts(half, meta, own, arrived, places, weights, shared):
    blocks = meta.shape[0]
    experts, units, width = weights[0].shape
    count = own.shape[0]
    group = next(g for g in (8, 4, 2, 1) if experts % g == 0)
    once = pl.Buffered(1)

    def whole(array):
        return pl.BlockSpec(
            array.shape, lambda o, i: (0,) * array.ndim, pipeline_mode=once
        )

    pair = 2 if group % 2 == 0 else 1
    steps = group // pair
    weight_spec = pl.BlockSpec((pair, units, width), lambda o, i: (o * steps + i, 0, 0))
    out_shape = (2, count, width // 4)
    out_spec = pl.BlockSpec(out_shape, lambda o, i: (0, 0, 0), pipeline_mode=once)
    return pl.pallas_call(
        functools.partial(expert_kernel, blocks, group, places),
        grid=(experts // group, steps),
        in_specs=[
            pl.BlockSpec(memory_space=pltpu.SMEM),
            pl.BlockSpec((blocks, 2, group, count), lambda o, i: (0, 0, o, 0)),
            whole(own),
            *[whole(a) for a in arrived],
            weight_spec,
            weight_spec,
            weight_spec,
            *[whole(s) for s in shared],
        ],
        out_specs=[out_spec] * (2 * len(PIECES)),
        out_shape=[jax.ShapeDtypeStruct(out_shape, jnp.float32)] * len(PIECES)
        + [jax.ShapeDtypeStruct(out_shape, jnp.bfloat16)] * len(PIECES),
        scratch_shapes=[
            pltpu.VMEM((blocks, count, width), jnp.bfloat16),
            pltpu.VMEM((group, blocks * CAP, width), jnp.bfloat16),
            pltpu.VMEM((blocks, group, CAP, width), jnp.bfloat16),
            pltpu.VMEM((blocks, count, width), jnp.float32),
        ],
        compiler_params=pltpu.CompilerParams(
            dimension_semantics=("arbitrary", "arbitrary"), vmem_limit_bytes=60 * 2**20
        ),
    )(half, meta, own, *arrived, *weights, *shared)


def gathered_plan(tokens, experts, gates, w_gate, w_up, w_down, shared_gate, shared_up, shared_down):
    count, width = tokens.shape
    topk = experts.shape[1]
    exp_local = w_gate.shape[0]
    blocks = lax.axis_size("blk")
    reps = lax.axis_size("rep")
    blk, half, rep = lax.axis_index("blk"), lax.axis_index("half"), lax.axis_index("rep")

    piece = lax.dynamic_slice_in_dim(tokens, half * (count // 2), count // 2, 0)
    from_x, from_y = send(piece, "blk", 1), send(piece, "blk", 2)

    turned = experts.T
    names = jnp.arange(E, dtype=jnp.int32)[:, None]
    named = jnp.zeros((E, count), jnp.float32)
    gate_of = jnp.zeros((E, count), jnp.float32)
    gates_turned = gates.astype(jnp.float32).T
    for j in range(topk):
        same = names == turned[j][None, :]
        named = jnp.where(same, 1.0, named)
        gate_of = jnp.where(same, gates_turned[j][None, :], gate_of)
    index = jnp.arange(count, dtype=jnp.int32)
    earlier = (index[:, None] < index[None, :]).astype(jnp.bfloat16)
    ranks = jnp.dot(named.astype(jnp.bfloat16), earlier, preferred_element_type=jnp.float32)
    slots = jnp.where(named > 0, ranks, -1.0)
    meta = jnp.stack([slots, gate_of]).astype(jnp.bfloat16)

    quarter = count // 4
    from_x, from_y, meta = lax.optimization_barrier((from_x, from_y, meta))
    top, low = send(from_x[:quarter], "blk", 2), send(from_y[quarter:], "blk", 1)

    def for_block(b):
        return lax.dynamic_slice_in_dim(meta, b * exp_local, exp_local, 1)

    metas = [for_block(blk)]
    for k in range(1, blocks):
        metas.append(send(for_block(target(blk, k, blocks)), "blk", k))
    mine = (from_x, from_y, top, low)
    where = ((1, 0), (2, 0), (3, 0), (3, quarter))
    arrived = mine + tuple(send(value, "half", 1) for value in mine)
    places = tuple((k, False, first) for k, first in where)
    places += tuple((k, True, first) for k, first in where)

    outs = run_experts(
        half.astype(jnp.int32).reshape(1),
        jnp.stack(metas).astype(jnp.float32),
        tokens,
        arrived,
        places,
        (w_gate, w_up, w_down),
        (shared_gate, shared_up, shared_down),
    )
    keeps, sends = outs[:len(PIECES)], outs[len(PIECES):]
    peers = [send(value, "half", 1) for value in sends]

    def joined(p, j):
        return keeps[p][j] + peers[p][j].astype(jnp.float32)

    def packed(p):
        return (keeps[p] + peers[p].astype(jnp.float32)).astype(jnp.bfloat16)

    got_x, got_y = send(packed(FIRST_X), "blk", 1), send(packed(FIRST_Y), "blk", 2)
    onward_x = (joined(LAST_X, 1) + got_x[1].astype(jnp.float32)).astype(jnp.bfloat16)
    onward_y = (joined(LAST_Y, 1) + got_y[1].astype(jnp.float32)).astype(jnp.bfloat16)
    late_x, late_y = send(onward_x, "blk", 2), send(onward_y, "blk", 1)
    left = joined(LAST_X, 0) + got_x[0].astype(jnp.float32) + late_x.astype(jnp.float32)
    right = joined(LAST_Y, 0) + got_y[0].astype(jnp.float32) + late_y.astype(jnp.float32)
    total = jnp.concatenate([left, right], axis=1)
    side = total.shape[1] // reps

    def for_rep(r):
        return lax.dynamic_slice_in_dim(total, r * side, side, 1)

    result = for_rep(rep)
    for k in range(reps - 1, 0, -1):
        share = for_rep(target(rep, k, reps)).astype(jnp.bfloat16)
        result = result + send(share, "rep", k).astype(jnp.float32)
    return result.astype(jnp.bfloat16)


def hidden_units(token_rows, gate_matrix, up_weight):
    gate_values = jnp.einsum(
        "kan,ktn->kat", token_rows, gate_matrix, preferred_element_type=jnp.float32
    )
    raised_rows = jnp.einsum(
        "kan,ktn->kat", token_rows, up_weight, preferred_element_type=jnp.float32
    )
    return (jax.nn.silu(gate_values) * raised_rows).astype(jnp.bfloat16)


def place_slots(flat, ranks, block_size, which, slot_count):
    inside = ranks // block_size == which
    local = jnp.where(inside, flat * block_size + ranks % block_size, -1)
    return local[:, None] == jnp.arange(slot_count, dtype=jnp.int32)[None, :]


def slotted_plan(tokens, experts, gates, w_gate, w_up, w_down, shared_gate, shared_up, shared_down):
    token_count = tokens.shape[0]
    width = tokens.shape[1]
    topk = experts.shape[1]
    exp_local = w_gate.shape[0]
    blk_count = lax.axis_size("blk")
    slot_block = CAP // lax.axis_size("rep")
    member_rep = lax.axis_index("rep")
    flat = experts.reshape(-1)
    onehot = (flat[:, None] == jnp.arange(E, dtype=jnp.int32)[None, :]).astype(jnp.int32)
    before = jnp.cumsum(onehot, axis=0) - onehot
    ranks = jnp.sum(before * onehot, axis=1)
    placing = place_slots(flat, ranks, slot_block, member_rep, E * slot_block).reshape(
        token_count, topk, -1
    )
    weighting = jnp.sum(
        placing.astype(jnp.float32) * gates.astype(jnp.float32)[:, :, None], axis=1
    ).astype(jnp.bfloat16)
    selector = jnp.any(placing, axis=1).astype(jnp.bfloat16)
    filled = jnp.einsum("ts,td->sd", selector, tokens, preferred_element_type=jnp.float32).astype(
        jnp.bfloat16
    )
    filled = filled.reshape(E, 1, slot_block, width)
    arrived = lax.all_to_all(filled, "blk", split_axis=0, concat_axis=1, tiled=True)
    token_rows = arrived.reshape(exp_local, -1, width)
    every_hidden = hidden_units(lax.all_gather(token_rows, "rep", axis=1, tiled=True), w_gate, w_up)
    mine = lax.all_to_all(every_hidden, "rep", split_axis=1, concat_axis=2, tiled=True)
    partial_value = jnp.einsum(
        "otv,ovj->otj",
        mine,
        lax.all_gather(w_down, "rep", axis=1, tiled=True),
        preferred_element_type=jnp.float32,
    )
    block_out = partial_value.astype(jnp.bfloat16).reshape(exp_local, blk_count, slot_block, width)
    returned = lax.all_to_all(block_out, "blk", split_axis=1, concat_axis=0, tiled=True)
    returned = returned.reshape(E * slot_block, width)
    routed = jnp.dot(weighting, returned, preferred_element_type=jnp.float32)
    shared_hidden = (
        jax.nn.silu(
            jnp.einsum("td,sd->ts", tokens, shared_gate, preferred_element_type=jnp.float32)
        )
        * jnp.einsum("td,sd->ts", tokens, shared_up, preferred_element_type=jnp.float32)
    ).astype(jnp.bfloat16)
    shared_output = jnp.dot(shared_hidden, shared_down, preferred_element_type=jnp.float32)
    routed_share = lax.psum_scatter(routed, ("half", "rep"), scatter_dimension=1, tiled=True)
    shared_share = lax.psum_scatter(shared_output, ("half", "rep"), scatter_dimension=1, tiled=True)
    total = routed_share + shared_share
    return total.astype(jnp.bfloat16)


def per_device(*args):
    tokens, w_gate = args[0], args[3]
    blocks = lax.axis_size("blk")
    gathered_rows = blocks * tokens.shape[0]
    slot_rows = w_gate.shape[0] * blocks * CAP
    if gathered_rows <= slot_rows and lax.axis_size("half") == 2 and blocks == 4:
        return gathered_plan(*args)
    return slotted_plan(*args)


def solution(mesh):
    return jax.shard_map(
        per_device,
        mesh=mesh,
        in_specs=(
            P("blk", None),
            P("blk", None),
            P("blk", None),
            P("blk", ("half", "rep"), None),
            P("blk", ("half", "rep"), None),
            P("blk", ("half", "rep"), None),
            P(("half", "rep"), None),
            P(("half", "rep"), None),
            P(("half", "rep"), None),
        ),
        out_specs=P("blk", ("half", "rep")),
        check_vma=False,
    )
```
